32 devices in a mesh: dp: 1 (over z), cy: 4 (over y), cx: 8 (over x, core).
Axes of the slice: x: 4, y: 4, z: 1, core: 2. Of those that a mesh axis runs over, the one named last changes fastest.
The devices are a block of a 4x4x8 slice.
Arguments:
- q: bfloat16 [4096, 32, 128], P(('dp', 'cy', 'cx'))
- k: bfloat16 [4096, 8, 128], P(('dp', 'cy', 'cx'))
- v: bfloat16 [4096, 8, 128], P(('dp', 'cy', 'cx'))
Outputs:
- output: bfloat16 [4096, 32, 128], P(('dp', 'cy', 'cx'))
All inputs are finite; a program needn't handle non-finite values.
Results may differ from the reference program's by a relative error of at most 0.00348894.
Values are sent between devices in bfloat16 or wider.
A program may use at most 768 MiB of HBM per device.

```python
import jax
import jax.numpy as jnp
from jax import lax

SEQ = 4096
NDEV = 32
HEADS = 32
KV_HEADS = 8
HEAD_DIM = 128

SPAN = SEQ // (2 * NDEV)
NEG = -1.0e30


def positions():
    i = jnp.arange(SEQ)
    blk = i // (2 * SPAN)
    j = i % (2 * SPAN)
    return jnp.where(j < SPAN, blk * SPAN + j, (2 * NDEV - 1 - blk) * SPAN + j - SPAN)


def setup_inputs(seed: int = 0, part: int = 0) -> dict:
    key = jax.random.fold_in(jax.random.key(seed), part)
    kq, kk, kv, ko = jax.random.split(key, 4)
    q = jax.random.normal(kq, (SEQ, HEADS, HEAD_DIM), jnp.float32)
    k = jax.random.normal(kk, (SEQ, KV_HEADS, HEAD_DIM), jnp.float32)
    off = jax.random.normal(ko, (2 * NDEV, 1, KV_HEADS, HEAD_DIM), jnp.float32)
    v = 0.5 * jax.random.normal(kv, (2 * NDEV, SPAN, KV_HEADS, HEAD_DIM), jnp.float32) + off
    v = v.reshape(SEQ, KV_HEADS, HEAD_DIM)
    return {'q': q.astype(jnp.bfloat16), 'k': k.astype(jnp.bfloat16), 'v': v.astype(jnp.bfloat16)}


def reference(q, k, v):
    rep = HEADS // KV_HEADS
    scale = HEAD_DIM ** -0.5
    pos = positions().reshape(2 * NDEV, SPAN)
    qc = q.reshape(2 * NDEV, SPAN, KV_HEADS, rep, HEAD_DIM)
    kc = k.reshape(2 * NDEV, SPAN, KV_HEADS, HEAD_DIM)
    vc = v.reshape(2 * NDEV, SPAN, KV_HEADS, HEAD_DIM)

    def one_query_span(xs):
        qb, pq = xs
        qf = qb.astype(jnp.float32)

        def step(carry, ys):
            m, l, acc = carry
            kb, vb, pk = ys
            s = jnp.einsum('qgrd,kgd->grqk', qf, kb.astype(jnp.float32)) * scale
            mask = pk[None, :] <= pq[:, None]
            s = jnp.where(mask, s, NEG)
            mn = jnp.maximum(m, jnp.max(s, axis=-1))
            p = jnp.where(mask, jnp.exp(s - mn[..., None]), 0.0)
            alpha = jnp.exp(m - mn)
            l = alpha * l + jnp.sum(p, axis=-1)
            pv = jnp.einsum('grqk,kgd->grqd', p.astype(jnp.bfloat16).astype(jnp.float32), vb.astype(jnp.float32))
            acc = alpha[..., None] * acc + pv
            return (mn, l, acc), None

        init = (jnp.full((KV_HEADS, rep, SPAN), NEG, jnp.float32),
                jnp.zeros((KV_HEADS, rep, SPAN), jnp.float32),
                jnp.zeros((KV_HEADS, rep, SPAN, HEAD_DIM), jnp.float32))
        (m, l, acc), _ = lax.scan(step, init, (kc, vc, pos))
        o = (acc / l[..., None]).astype(jnp.bfloat16)
        return o.transpose(2, 0, 1, 3).reshape(SPAN, HEADS, HEAD_DIM)

    out = lax.map(one_query_span, (qc, pos))
    return out.reshape(SEQ, HEADS, HEAD_DIM)
```

```python
import functools
import math

import jax
import jax.numpy as jnp
from jax import lax
from jax.experimental import pallas as pl
from jax.experimental.pallas import tpu as pltpu
from jax.sharding import PartitionSpec as P

NEG = -1.0e30
MESH = pl.DeviceIdType.MESH
F32 = jnp.float32


def kernel(n, c2, q_hbm, kv_hbm, out_hbm, kvbuf, qbuf, vt, acc, mref, lref, ostage,
           ks, kr, qs, qr, gs, gr, os, orx):
    ng, rep, t2, hd = q_hbm.shape
    c = t2 // 2
    nb2 = 2 * n
    half = n * t2
    cols = rep * t2
    dp = lax.axis_index('dp')
    y = lax.axis_index('cy')
    cx = lax.axis_index('cx')
    x = cx // 2
    core = cx % 2
    row_core = core == 0
    own = jnp.where(row_core, y, x)
    pos = jnp.where(row_core, x, y)
    g_me = jnp.where(row_core, x, n + y)

    barrier = pltpu.get_barrier_semaphore()
    cnt = 0
    for d in range(1, 2 * n):
        pl.semaphore_signal(barrier, inc=1, device_id=(dp, y, (cx + d) % (2 * n)), device_id_type=MESH)
        cnt += 1
    for d in range(1, n):
        for cc in range(2):
            pl.semaphore_signal(barrier, inc=1, device_id=(dp, (y + d) % n, 2 * x + cc), device_id_type=MESH)
            cnt += 1
    pl.semaphore_wait(barrier, cnt)

    order = (2, 1, 3, 0) if n == 4 else tuple(range(n))[::-1]

    def spread(fn, sends, recv):
        waits = []
        i = 0
        for d in order:
            for lay in range(2):
                u = x if lay == 0 else y
                j = (u + d) % n
                g = j + lay * n
                dev = (dp, y, 2 * j) if lay == 0 else (dp, j, 2 * x + 1)
                grp = y if lay == 0 else x
                for h in range(2):
                    src, dst = fn(g, grp, u, h)
                    cp = pltpu.make_async_remote_copy(src_ref=src, dst_ref=dst, send_sem=sends.at[i], recv_sem=recv.at[0],
                                                      device_id=dev, device_id_type=MESH)
                    if d == 0:
                        lc = pltpu.make_async_copy(src, dst, recv.at[0])
                        pl.when(core == lay)(lc.start)
                        pl.when(core != lay)(cp.start)
                        waits.append(lambda cp=cp, lay=lay: pl.when(core != lay)(cp.wait_send))
                    else:
                        cp.start()
                        waits.append(cp.wait_send)
                    i += 1
        return waits

    def kv_piece(g, grp, u, h):
        blk = u if h == 0 else nb2 - 1 - u
        sub = core if h == 0 else 1 - core
        off = pl.multiple_of(blk * t2 + sub * c, c)
        return kv_hbm.at[g, :, pl.ds(h * c, c)], kvbuf.at[grp, :, pl.ds(off, c)]

    def q_piece(g, grp, u, h):
        blk = u if h == 0 else nb2 - 1 - u
        sub = core if h == 0 else 1 - core
        off = pl.multiple_of(sub * c, c)
        return q_hbm.at[g, :, pl.ds(h * c, c)], qbuf.at[blk, :, pl.ds(off, c)]

    waits = spread(kv_piece, ks, kr)
    waits += spread(q_piece, qs, qr)

    def me_wait(ref, sem):
        pltpu.make_async_copy(ref, ref, sem).wait()

    def peer(p):
        return (dp, jnp.where(row_core, p, y), jnp.where(row_core, 2 * x, 2 * p + 1))

    me_wait(kvbuf.at[own], kr.at[0])
    for i, d in enumerate((1, 3, 2) if n == 4 else range(1, n)):
        p = (own + d) % n
        for h in range(2):
            part = kvbuf.at[own, :, pl.ds(h * half, half)]
            cp = pltpu.make_async_remote_copy(src_ref=part, dst_ref=part, send_sem=gs.at[2 * i + h],
                                              recv_sem=gr.at[2 * own + h], device_id=peer(p), device_id_type=MESH)
            if h == 0:
                cp.start()
                waits.append(cp.wait_send)
            else:
                need = jnp.logical_or(core == 1, own > p)
                pl.when(need)(cp.start)
                waits.append(lambda cp=cp, need=need: pl.when(need)(cp.wait_send))

    def turn_v(t, base):
        vt[:, pl.ds(base, half)] = kvbuf[t, 1, pl.ds(base, half), :].T

    def attend(a, t, base, nk, diag, first):
        k = kvbuf[t, 0, pl.ds(base, nk), :]
        v = vt[:, pl.ds(base, nk)]
        q = qbuf[a].reshape(cols, hd)
        s = lax.dot_general(k, q, (((1,), (1,)), ((), ())), preferred_element_type=F32)
        if diag:
            key = lax.broadcasted_iota(jnp.int32, (t2, cols), 0)
            row = lax.broadcasted_iota(jnp.int32, (t2, cols), 1) % t2
            last = jnp.where(key <= row, s[nk - t2:], NEG)
            s = last if nk == t2 else jnp.concatenate([s[:nk - t2], last], axis=0)
        mx = jnp.max(s, axis=0, keepdims=True)
        if not first:
            mp = mref[a]
            mx = jnp.maximum(mp, mx)
            alpha = jnp.exp2((mp - mx) * c2)
        mref[a] = mx
        p = jnp.exp2((s - mx) * c2)
        ls = jnp.sum(p, axis=0, keepdims=True)
        pv = lax.dot_general(v, p.astype(jnp.bfloat16), (((1,), (0,)), ((), ())), preferred_element_type=F32)
        if first:
            lref[a] = ls
            acc[a] = pv
        else:
            lref[a] = alpha * lref[a] + ls
            acc[a] = alpha * acc[a] + pv

    me_wait(qbuf, qr.at[0])
    turn_v(own, 0)
    turn_v(own, half)
    for a in range(nb2):
        if a >= n:
            attend(a, own, 0, half, False, True)
            attend(a, own, half, (a - n + 1) * t2, True, False)
        else:
            attend(a, own, 0, (a + 1) * t2, True, True)

    def finish(a):
        o = acc[a] * (1.0 / lref[a])
        for r in range(rep):
            ostage[a, r] = o[:, r * t2:(r + 1) * t2].T.astype(jnp.bfloat16)

    def o_copies(a, h):
        first_half = a < n
        u = jnp.where(first_half, a, nb2 - 1 - a)
        cc = jnp.where(first_half, h, 1 - h)
        dev = (dp, jnp.where(row_core, y, u), jnp.where(row_core, 2 * u, 2 * x) + cc)
        off = pl.multiple_of(jnp.where(first_half, 0, c), c)
        src = ostage.at[a, :, pl.ds(h * c, c)]
        dst = out_hbm.at[g_me, :, pl.ds(off, c)]
        mine = jnp.logical_and(u == pos, cc == core)
        rc = pltpu.make_async_remote_copy(src_ref=src, dst_ref=dst, send_sem=os.at[2 * a + h], recv_sem=orx.at[0],
                                          device_id=dev, device_id_type=MESH)
        return mine, pltpu.make_async_copy(src, dst, orx.at[0]), rc

    def group(i, carry):
        f = jnp.where(i == 0, n - 1, jnp.where(i == 1, 1, 2)) if n == 4 else i + 1
        t = (own + f) % n
        need = jnp.logical_or(core == 1, t > own)
        me_wait(kvbuf.at[t, :, pl.ds(0, half)], gr.at[2 * t])
        turn_v(t, 0)

        @pl.when(need)
        def _():
            me_wait(kvbuf.at[t, :, pl.ds(half, half)], gr.at[2 * t + 1])
            turn_v(t, half)

        def block(ii, carry):
            a = nb2 - 1 - ii
            hi = a >= n
            am = a % n

            @pl.when(hi)
            def _():
                attend(a, t, 0, half, False, False)
            before = jnp.where(hi, t > own, t < own).astype(jnp.int32)
            cntb = jnp.where(row_core, n * before, am + before)
            base = pl.multiple_of(jnp.where(hi, half, 0), half)
            for nb in range(1, n + 1):
                @pl.when(cntb == nb)
                def _(nb=nb):
                    attend(a, t, base, nb * t2, False, False)

            @pl.when(i == n - 2)
            def _():
                finish(a)
                for h in range(2):
                    mine, lc, rc = o_copies(a, h)
                    pl.when(mine)(lc.start)
                    pl.when(jnp.logical_not(mine))(rc.start)
            return carry

        return lax.fori_loop(0, nb2, block, carry)

    lax.fori_loop(0, n - 1, group, 0)

    for w in waits:
        w()

    def drain(a, carry):
        for h in range(2):
            mine, _, rc = o_copies(a, h)
            pl.when(jnp.logical_not(mine))(rc.wait_send)
        return carry

    lax.fori_loop(0, nb2, drain, 0)
    me_wait(out_hbm, orx.at[0])


def solution(mesh):
    n = mesh.shape['cy']
    assert mesh.shape['cx'] == 2 * n
    spec = P(('dp', 'cy', 'cx'))

    def local(q, k, v):
        t, nh, hd = q.shape
        ng = k.shape[1]
        assert ng == 2 * n
        rep = nh // ng
        c2 = hd ** -0.5 * math.log2(math.e)
        qh = q.transpose(1, 0, 2).reshape(ng, rep, t, hd)
        kv = jnp.stack([k.transpose(1, 0, 2), v.transpose(1, 0, 2)], axis=1)
        dma = pltpu.SemaphoreType.DMA
        o = pl.pallas_call(
            functools.partial(kernel, n, c2),
            out_shape=jax.ShapeDtypeStruct((ng, rep, t, hd), q.dtype),
            in_specs=[pl.BlockSpec(memory_space=pl.ANY)] * 2,
            out_specs=pl.BlockSpec(memory_space=pl.ANY),
            scratch_shapes=[
                pltpu.VMEM((n, 2, 2 * n * t, hd), k.dtype),
                pltpu.VMEM((2 * n, rep, t, hd), q.dtype),
                pltpu.VMEM((hd, 2 * n * t), v.dtype),
                pltpu.VMEM((2 * n, hd, rep * t), F32),
                pltpu.VMEM((2 * n, 1, rep * t), F32),
                pltpu.VMEM((2 * n, 1, rep * t), F32),
                pltpu.VMEM((2 * n, rep, t, hd), q.dtype),
                dma((4 * n,)), dma((1,)), dma((4 * n,)), dma((1,)),
                dma((2 * n - 2,)), dma((2 * n,)), dma((4 * n,)), dma((1,)),
            ],
            compiler_params=pltpu.CompilerParams(collective_id=0, has_side_effects=True,
                                                 vmem_limit_bytes=56 * 1024 * 1024),
        )(qh, kv)
        return o.reshape(nh, t, hd).transpose(1, 0, 2)

    return jax.shard_map(local, mesh=mesh, in_specs=(spec, spec, spec), out_specs=spec, check_vma=False)
```

```python
import functools
import math

import jax
import jax.numpy as jnp
from jax import lax
from jax.experimental import pallas as pl
from jax.experimental.pallas import tpu as pltpu
from jax.sharding import PartitionSpec as P

NEG = -1.0e30
MESH = pl.DeviceIdType.MESH
F32 = jnp.float32


def kernel(n, c2, q_hbm, k_hbm, v_hbm, out_hbm, kvbuf, qbuf, qt, vt, s0, s1, s2, s3, x0, x1, x2, x3, acc, mref, lref, ostage,
           ks, kr, qs, qr, gs, gr, os, orx):
    t2, ng, rep, hd = q_hbm.shape
    c = t2 // 2
    nb2 = 2 * n
    half = n * t2
    cols = rep * t2
    dp = lax.axis_index('dp')
    y = lax.axis_index('cy')
    cx = lax.axis_index('cx')
    x = cx // 2
    core = cx % 2
    row_core = core == 0
    own = jnp.where(row_core, y, x)
    pos = jnp.where(row_core, x, y)
    g_me = jnp.where(row_core, x, n + y)

    barrier = pltpu.get_barrier_semaphore()
    cnt = 0
    for d in range(1, 2 * n):
        pl.semaphore_signal(barrier, inc=1, device_id=(dp, y, (cx + d) % (2 * n)), device_id_type=MESH)
        cnt += 1
    for d in range(1, n):
        for cc in range(2):
            pl.semaphore_signal(barrier, inc=1, device_id=(dp, (y + d) % n, 2 * x + cc), device_id_type=MESH)
            cnt += 1
    pl.semaphore_wait(barrier, cnt)

    order = (2, 1, 3, 0) if n == 4 else tuple(range(n))[::-1]

    def spread(fn, sends, recv, split, parts):
        waits = []
        i = 0
        for d in order:
            for lay in range(2):
                u = x if lay == 0 else y
                j = (u + d) % n
                g = j + lay * n
                dev = (dp, y, 2 * j) if lay == 0 else (dp, j, 2 * x + 1)
                grp = y if lay == 0 else x
                for h in range(parts):
                    src, dst = fn(g, grp, u, h)
                    rsem = recv.at[u if split else 0]
                    cp = pltpu.make_async_remote_copy(src_ref=src, dst_ref=dst, send_sem=sends.at[i], recv_sem=rsem,
                                                      device_id=dev, device_id_type=MESH)
                    if d == 0:
                        lc = pltpu.make_async_copy(src, dst, rsem)
                        pl.when(core == lay)(lc.start)
                        pl.when(core != lay)(cp.start)
                        waits.append(lambda cp=cp, lay=lay: pl.when(core != lay)(cp.wait_send))
                    else:
                        cp.start()
                        waits.append(cp.wait_send)
                    i += 1
        return waits

    def kv_piece(g, grp, u, hw):
        h, w = hw % 2, hw // 2
        blk = u if h == 0 else nb2 - 1 - u
        sub = core if h == 0 else 1 - core
        off = pl.multiple_of(blk * t2 + sub * c, c)
        return (k_hbm, v_hbm)[w].at[g, pl.ds(h * c, c)], kvbuf.at[grp, w, pl.ds(off, c)]

    def q_piece(g, grp, u, h):
        blk = u if h == 0 else nb2 - 1 - u
        sub = core if h == 0 else 1 - core
        off = pl.multiple_of(sub * c, c)
        return q_hbm.at[pl.ds(h * c, c), g], qbuf.at[blk, pl.ds(off, c)]

    waits = spread(kv_piece, ks, kr, False, 4)
    waits += spread(q_piece, qs, qr, True, 2)

    def me_wait(ref, sem):
        pltpu.make_async_copy(ref, ref, sem).wait()

    def peer(p):
        return (dp, jnp.where(row_core, p, y), jnp.where(row_core, 2 * x, 2 * p + 1))

    def share_copies():
        for i, d in enumerate((1, 3, 2) if n == 4 else range(1, n)):
            p = (own + d) % n
            for h in range(2):
                part = kvbuf.at[own, :, pl.ds(h * half, half)]
                cp = pltpu.make_async_remote_copy(src_ref=part, dst_ref=part, send_sem=gs.at[2 * i + h],
                                                  recv_sem=gr.at[2 * own + h], device_id=peer(p), device_id_type=MESH)
                yield cp, True if h == 0 else jnp.logical_or(core == 1, own > p)

    def share():
        for cp, need in share_copies():
            pl.when(need)(cp.start)

    def turn_v(t, base):
        vt[:, pl.ds(base, half)] = kvbuf[t, 1, pl.ds(base, half), :].T

    s_bufs = (s0, s1, s2, s3)
    x_bufs = (x0, x1, x2, x3)

    def score(step, t, slot):
        q, b0, nb, diag, _ = step
        k = kvbuf[t, 0, pl.ds(b0 * t2, nb * t2), :]
        s = lax.dot_general(k, qt[q], (((1,), (0,)), ((), ())), preferred_element_type=F32)
        if diag:
            key = lax.broadcasted_iota(jnp.int32, (t2, cols), 0)
            row = lax.broadcasted_iota(jnp.int32, (t2, cols), 1) // rep
            tail = jnp.where(key <= row, s[(nb - 1) * t2:], NEG)
            s = tail if nb == 1 else jnp.concatenate([s[:(nb - 1) * t2], tail], axis=0)
        s_bufs[slot][pl.ds(0, nb * t2), :] = s
        x_bufs[slot][...] = jnp.max(s, axis=0, keepdims=True)

    def fold(step, slot):
        q, b0, nb, _, fresh = step
        s = s_bufs[slot][pl.ds(0, nb * t2), :]
        mx = x_bufs[slot][...]
        if not fresh:
            mp = mref[q]
            mx = jnp.maximum(mp, mx)
            alpha = jnp.exp2((mp - mx) * c2)
        mref[q] = mx
        p = jnp.exp2((s - mx) * c2)
        ls = jnp.sum(p, axis=0, keepdims=True)
        v = vt[:, pl.ds(b0 * t2, nb * t2)]
        pv = lax.dot_general(v, p.astype(jnp.bfloat16), (((1,), (0,)), ((), ())), preferred_element_type=F32)
        if fresh:
            lref[q] = ls
            acc[q] = pv
        else:
            lref[q] = alpha * lref[q] + ls
            acc[q] = alpha * acc[q] + pv

    def run(t, counts, own_group):
        plan = []
        for q, cnt in counts:
            b0 = 0
            while b0 < cnt:
                nb = min(4, cnt - b0)
                plan.append((q, b0, nb, own_group and b0 + nb == cnt, own_group and b0 == 0))
                b0 += nb
        for i in range(min(2, len(plan))):
            score(plan[i], t, i % 4)
        for i, step in enumerate(plan):
            if i + 2 < len(plan):
                score(plan[i + 2], t, (i + 2) % 4)
            fold(step, i % 4)

    def near(i):
        return jnp.where(i == 0, 0, jnp.where(i == 1, n - 1, i - 1))

    parts = (tuple(range(n)), tuple(range(n, n + n // 2)), tuple(range(n + n // 2, nb2)))

    def finish(a):
        o = acc[a] * (1.0 / lref[a])
        ostage[a] = o.T.astype(jnp.bfloat16).reshape(t2, rep, hd)

    def o_copies(a, h):
        first_half = a < n
        u = jnp.where(first_half, a, nb2 - 1 - a)
        cc = jnp.where(first_half, h, 1 - h)
        dev = (dp, jnp.where(row_core, y, u), jnp.where(row_core, 2 * u, 2 * x) + cc)
        off = pl.multiple_of(jnp.where(first_half, 0, c), c)
        src = ostage.at[a, pl.ds(h * c, c)]
        dst = out_hbm.at[pl.ds(off, c), g_me]
        mine = jnp.logical_and(u == pos, cc == core)
        rc = pltpu.make_async_remote_copy(src_ref=src, dst_ref=dst, send_sem=os.at[2 * a + h], recv_sem=orx.at[0],
                                          device_id=dev, device_id_type=MESH)
        return mine, pltpu.make_async_copy(src, dst, orx.at[0]), rc

    def send_out(a):
        finish(a)
        for h in range(2):
            mine, lc, rc = o_copies(a, h)
            pl.when(mine)(lc.start)
            pl.when(jnp.logical_not(mine))(rc.start)

    def turn_q(u):
        me_wait(qbuf.at[pl.ds(0, 2)], qr.at[u])
        for blk in (u, nb2 - 1 - u):
            qt[blk] = qbuf[blk].reshape(cols, hd).T

    def other(t, last, core_is, before):
        for part in parts:
            if core_is == 0:
                counts = [(q, (n if before else 0) if q < n else (n if before else nb2)) for q in part]
            else:
                counts = [(q, q + int(before == (q < n))) for q in part]
            run(t, counts, False)

            @pl.when(last)
            def _(part=part):
                lax.fori_loop(part[0], part[-1] + 1, lambda q, c: (send_out(q), c)[1], 0)

    me_wait(kvbuf.at[own], kr.at[0])
    share()
    turn_v(own, 0)
    turn_v(own, half)
    lax.fori_loop(0, n, lambda i, c: (turn_q((pos + near(i)) % n), c)[1], 0)
    run(own, [(q, q + 1) for q in range(nb2)], True)

    def group(i, carry):
        t = (own + near(i)) % n
        last = i == n - 1
        me_wait(kvbuf.at[t, :, pl.ds(0, half)], gr.at[2 * t])
        turn_v(t, 0)

        @pl.when(jnp.logical_or(core == 1, t > own))
        def _():
            me_wait(kvbuf.at[t, :, pl.ds(half, half)], gr.at[2 * t + 1])
            turn_v(t, half)

        for core_is in range(2):
            for before in (True, False):
                @pl.when(jnp.logical_and(core == core_is, (t < own) == before))
                def _(core_is=core_is, before=before):
                    other(t, last, core_is, before)
        return carry

    lax.fori_loop(1, n, group, 0)

    for w in waits:
        w()
    for cp, need in share_copies():
        pl.when(need)(cp.wait_send)

    def drain(a, carry):
        for h in range(2):
            mine, _, rc = o_copies(a, h)
            pl.when(jnp.logical_not(mine))(rc.wait_send)
        return carry

    lax.fori_loop(0, nb2, drain, 0)
    me_wait(out_hbm, orx.at[0])


def solution(mesh):
    n = mesh.shape['cy']
    assert mesh.shape['cx'] == 2 * n
    spec = P(('dp', 'cy', 'cx'))

    def local(q, k, v):
        t, nh, hd = q.shape
        ng = k.shape[1]
        assert ng == 2 * n
        rep = nh // ng
        c2 = hd ** -0.5 * math.log2(math.e)
        qh = q.reshape(t, ng, rep, hd)
        dma = pltpu.SemaphoreType.DMA
        o = pl.pallas_call(
            functools.partial(kernel, n, c2),
            out_shape=jax.ShapeDtypeStruct((t, ng, rep, hd), q.dtype),
            in_specs=[pl.BlockSpec(memory_space=pl.ANY)] * 3,
            out_specs=pl.BlockSpec(memory_space=pl.ANY),
            scratch_shapes=[
                pltpu.VMEM((n, 2, 2 * n * t, hd), k.dtype),
                pltpu.VMEM((2 * n, t, rep, hd), q.dtype),
                pltpu.VMEM((2 * n, hd, rep * t), q.dtype),
                pltpu.VMEM((hd, 2 * n * t), v.dtype),
                *[pltpu.VMEM((4 * t, rep * t), F32)] * 4,
                *[pltpu.VMEM((1, rep * t), F32)] * 4,
                pltpu.VMEM((2 * n, hd, rep * t), F32),
                pltpu.VMEM((2 * n, 1, rep * t), F32),
                pltpu.VMEM((2 * n, 1, rep * t), F32),
                pltpu.VMEM((2 * n, t, rep, hd), q.dtype),
                dma((8 * n,)), dma((1,)), dma((4 * n,)), dma((n,)),
                dma((2 * n - 2,)), dma((2 * n,)), dma((4 * n,)), dma((1,)),
            ],
            compiler_params=pltpu.CompilerParams(collective_id=0, has_side_effects=True,
                                                 vmem_limit_bytes=56 * 1024 * 1024),
        )(qh, k.transpose(1, 0, 2), v.transpose(1, 0, 2))
        return o.reshape(t, nh, hd)

    return jax.shard_map(local, mesh=mesh, in_specs=(spec, spec, spec), out_specs=spec, check_vma=False)
```

```python
import functools
import math

import jax
import jax.numpy as jnp
from jax import lax
from jax.experimental import pallas as pl
from jax.experimental.pallas import tpu as pltpu
from jax.sharding import PartitionSpec as P

NEG = -1.0e30
MESH = pl.DeviceIdType.MESH
F32 = jnp.float32


def kernel(n, c2, q_hbm, k_hbm, v_hbm, out_hbm, kraw, wide, ksend, ksem, kvbuf, qbuf, qt, vt, s0, s1, s2, s3, x0, x1, x2, x3, acc, mref, lref, ostage,
           ks, kr, qs, qr, gs, gr, os, orx):
    t2, ng, rep, hd = q_hbm.shape
    c = t2 // 2
    nb2 = 2 * n
    half = n * t2
    cols = rep * t2
    dp = lax.axis_index('dp')
    y = lax.axis_index('cy')
    cx = lax.axis_index('cx')
    x = cx // 2
    core = cx % 2
    row_core = core == 0
    own = jnp.where(row_core, y, x)
    pos = jnp.where(row_core, x, y)
    g_me = jnp.where(row_core, x, n + y)

    barrier = pltpu.get_barrier_semaphore()
    cnt = 0
    for d in range(1, 2 * n):
        pl.semaphore_signal(barrier, inc=1, device_id=(dp, y, (cx + d) % (2 * n)), device_id_type=MESH)
        cnt += 1
    for d in range(1, n):
        for cc in range(2):
            pl.semaphore_signal(barrier, inc=1, device_id=(dp, (y + d) % n, 2 * x + cc), device_id_type=MESH)
            cnt += 1

    loads = [pltpu.make_async_copy(src, kraw.at[w], ksem.at[w]) for w, src in enumerate((k_hbm, v_hbm))]
    for cp in loads:
        cp.start()
    for w, cp in enumerate(loads):
        cp.wait()
        wide[w] = kraw[w].astype(F32).reshape(t2 * ng, hd)
        for g in range(ng):
            ksend[w, g] = wide[w, pl.ds(g, t2, stride=ng), :].astype(jnp.bfloat16)
    pl.semaphore_wait(barrier, cnt)

    order = (2, 1, 3, 0) if n == 4 else tuple(range(n))[::-1]

    def spread(fn, sends, recv, split, parts):
        waits = []
        i = 0
        for d in order:
            for lay in range(2):
                u = x if lay == 0 else y
                j = (u + d) % n
                g = j + lay * n
                dev = (dp, y, 2 * j) if lay == 0 else (dp, j, 2 * x + 1)
                grp = y if lay == 0 else x
                for h in range(parts):
                    src, dst = fn(g, grp, u, h)
                    rsem = recv.at[u if split else 0]
                    cp = pltpu.make_async_remote_copy(src_ref=src, dst_ref=dst, send_sem=sends.at[i], recv_sem=rsem,
                                                      device_id=dev, device_id_type=MESH)
                    if d == 0:
                        lc = pltpu.make_async_copy(src, dst, rsem)
                        pl.when(core == lay)(lc.start)
                        pl.when(core != lay)(cp.start)
                        waits.append(lambda cp=cp, lay=lay: pl.when(core != lay)(cp.wait_send))
                    else:
                        cp.start()
                        waits.append(cp.wait_send)
                    i += 1
        return waits

    def kv_piece(g, grp, u, hw):
        h, w = hw % 2, hw // 2
        blk = u if h == 0 else nb2 - 1 - u
        sub = core if h == 0 else 1 - core
        off = pl.multiple_of(blk * t2 + sub * c, c)
        return ksend.at[w, g, pl.ds(h * c, c)], kvbuf.at[grp, w, pl.ds(off, c)]

    def q_piece(g, grp, u, h):
        blk = u if h == 0 else nb2 - 1 - u
        sub = core if h == 0 else 1 - core
        off = pl.multiple_of(sub * c, c)
        return q_hbm.at[pl.ds(h * c, c), g], qbuf.at[blk, pl.ds(off, c)]

    waits = spread(kv_piece, ks, kr, False, 4)
    waits += spread(q_piece, qs, qr, True, 2)

    def me_wait(ref, sem):
        pltpu.make_async_copy(ref, ref, sem).wait()

    def peer(p):
        return (dp, jnp.where(row_core, p, y), jnp.where(row_core, 2 * x, 2 * p + 1))

    def hand_on(t, h, d, sem):
        p = (own + d) % n
        part = kvbuf.at[t, :, pl.ds(h * half, half)]
        cp = pltpu.make_async_remote_copy(src_ref=part, dst_ref=part, send_sem=gs.at[sem], recv_sem=gr.at[2 * t + h],
                                          device_id=peer(p), device_id_type=MESH)
        return cp, True if h == 0 else jnp.logical_or(core == 1, t > p)

    def share_copies():
        return [hand_on(own, h, d, sem) for sem, (h, d) in enumerate(((0, 1), (1, n - 1), (1, 1), (0, n - 1)))]

    prev, after = (own + n - 1) % n, (own + 1) % n

    def relay_copies():
        return [hand_on(prev, 0, 1, 4), hand_on(after, 1, n - 1, 5)]

    def relay():
        for (cp, need), t, h in zip(relay_copies(), (prev, after), (0, 1)):
            @pl.when(need)
            def _(cp=cp, t=t, h=h):
                me_wait(kvbuf.at[t, :, pl.ds(h * half, half)], gr.at[2 * t + h])
                cp.start()

    def share():
        for cp, need in share_copies():
            pl.when(need)(cp.start)

    def turn_v(t, base):
        vt[:, pl.ds(base, half)] = kvbuf[t, 1, pl.ds(base, half), :].T

    s_bufs = (s0, s1, s2, s3)
    x_bufs = (x0, x1, x2, x3)

    def score(step, t, slot):
        q, b0, nb, diag, _ = step
        k = kvbuf[t, 0, pl.ds(b0 * t2, nb * t2), :]
        s = lax.dot_general(k, qt[q], (((1,), (0,)), ((), ())), preferred_element_type=F32)
        if diag:
            key = lax.broadcasted_iota(jnp.int32, (t2, cols), 0)
            row = lax.broadcasted_iota(jnp.int32, (t2, cols), 1) // rep
            tail = jnp.where(key <= row, s[(nb - 1) * t2:], NEG)
            s = tail if nb == 1 else jnp.concatenate([s[:(nb - 1) * t2], tail], axis=0)
        s_bufs[slot][pl.ds(0, nb * t2), :] = s
        x_bufs[slot][...] = jnp.max(s, axis=0, keepdims=True)

    def fold(step, slot):
        q, b0, nb, _, fresh = step
        s = s_bufs[slot][pl.ds(0, nb * t2), :]
        mx = x_bufs[slot][...]
        if not fresh:
            mp = mref[q]
            mx = jnp.maximum(mp, mx)
            alpha = jnp.exp2((mp - mx) * c2)
        mref[q] = mx
        p = jnp.exp2((s - mx) * c2)
        ls = jnp.sum(p, axis=0, keepdims=True)
        v = vt[:, pl.ds(b0 * t2, nb * t2)]
        pv = lax.dot_general(v, p.astype(jnp.bfloat16), (((1,), (0,)), ((), ())), preferred_element_type=F32)
        if fresh:
            lref[q] = ls
            acc[q] = pv
        else:
            lref[q] = alpha * lref[q] + ls
            acc[q] = alpha * acc[q] + pv

    def run(t, counts, own_group):
        plan = []
        for q, cnt in counts:
            b0 = 0
            while b0 < cnt:
                nb = min(4, cnt - b0)
                plan.append((q, b0, nb, own_group and b0 + nb == cnt, own_group and b0 == 0))
                b0 += nb
        for i in range(min(2, len(plan))):
            score(plan[i], t, i % 4)
        for i, step in enumerate(plan):
            if i + 2 < len(plan):
                score(plan[i + 2], t, (i + 2) % 4)
            fold(step, i % 4)

    def near(i):
        return jnp.where(i == 0, 0, jnp.where(i == 1, n - 1, i - 1))

    parts = (tuple(range(n)), tuple(range(n, n + n // 2)), tuple(range(n + n // 2, nb2)))

    def finish(a):
        o = acc[a] * (1.0 / lref[a])
        ostage[a] = o.T.astype(jnp.bfloat16).reshape(t2, rep, hd)

    def o_copies(a, h):
        first_half = a < n
        u = jnp.where(first_half, a, nb2 - 1 - a)
        cc = jnp.where(first_half, h, 1 - h)
        dev = (dp, jnp.where(row_core, y, u), jnp.where(row_core, 2 * u, 2 * x) + cc)
        off = pl.multiple_of(jnp.where(first_half, 0, c), c)
        src = ostage.at[a, pl.ds(h * c, c)]
        dst = out_hbm.at[pl.ds(off, c), g_me]
        mine = jnp.logical_and(u == pos, cc == core)
        rc = pltpu.make_async_remote_copy(src_ref=src, dst_ref=dst, send_sem=os.at[2 * a + h], recv_sem=orx.at[0],
                                          device_id=dev, device_id_type=MESH)
        return mine, pltpu.make_async_copy(src, dst, orx.at[0]), rc

    def send_out(a):
        finish(a)
        for h in range(2):
            mine, lc, rc = o_copies(a, h)
            pl.when(mine)(lc.start)
            pl.when(jnp.logical_not(mine))(rc.start)

    def turn_q(u):
        me_wait(qbuf.at[pl.ds(0, 2)], qr.at[u])
        for blk in (u, nb2 - 1 - u):
            qt[blk] = qbuf[blk].reshape(cols, hd).T

    def other(t, last, core_is, before):
        for part in parts:
            if core_is == 0:
                counts = [(q, (n if before else 0) if q < n else (n if before else nb2)) for q in part]
            else:
                counts = [(q, q + int(before == (q < n))) for q in part]
            run(t, counts, False)

            @pl.when(last)
            def _(part=part):
                lax.fori_loop(part[0], part[-1] + 1, lambda q, c: (send_out(q), c)[1], 0)

    me_wait(kvbuf.at[own], kr.at[0])
    share()
    turn_v(own, 0)
    turn_v(own, half)
    lax.fori_loop(0, n, lambda i, c: (turn_q((pos + near(i)) % n), c)[1], 0)
    run(own, [(q, q + 1) for q in range(nb2)], True)

    relay()

    def group(i, carry):
        t = (own + near(i)) % n
        last = i == n - 1
        pl.when(i != 1)(lambda: me_wait(kvbuf.at[t, :, pl.ds(0, half)], gr.at[2 * t]))
        turn_v(t, 0)

        @pl.when(jnp.logical_or(core == 1, t > own))
        def _():
            relayed = jnp.logical_and(i == 2, jnp.logical_or(core == 1, t > prev))
            pl.when(jnp.logical_not(relayed))(lambda: me_wait(kvbuf.at[t, :, pl.ds(half, half)], gr.at[2 * t + 1]))
            turn_v(t, half)

        for core_is in range(2):
            for before in (True, False):
                @pl.when(jnp.logical_and(core == core_is, (t < own) == before))
                def _(core_is=core_is, before=before):
                    other(t, last, core_is, before)
        return carry

    lax.fori_loop(1, n, group, 0)

    for w in waits:
        w()
    for cp, need in share_copies() + relay_copies():
        pl.when(need)(cp.wait_send)

    def drain(a, carry):
        for h in range(2):
            mine, _, rc = o_copies(a, h)
            pl.when(jnp.logical_not(mine))(rc.wait_send)
        return carry

    lax.fori_loop(0, nb2, drain, 0)
    me_wait(out_hbm, orx.at[0])


def solution(mesh):
    n = mesh.shape['cy']
    assert n == 4 and mesh.shape['cx'] == 2 * n
    spec = P(('dp', 'cy', 'cx'))

    def local(q, k, v):
        t, nh, hd = q.shape
        ng = k.shape[1]
        assert ng == 2 * n
        rep = nh // ng
        c2 = hd ** -0.5 * math.log2(math.e)
        qh = q.reshape(t, ng, rep, hd)
        dma = pltpu.SemaphoreType.DMA
        o = pl.pallas_call(
            functools.partial(kernel, n, c2),
            out_shape=jax.ShapeDtypeStruct((t, ng, rep, hd), q.dtype),
            in_specs=[pl.BlockSpec(memory_space=pl.ANY)] * 3,
            out_specs=pl.BlockSpec(memory_space=pl.ANY),
            scratch_shapes=[
                pltpu.VMEM((2, t, ng, hd), k.dtype),
                pltpu.VMEM((2, t * ng, hd), F32),
                pltpu.VMEM((2, ng, t, hd), k.dtype),
                dma((2,)),
                pltpu.VMEM((n, 2, 2 * n * t, hd), k.dtype),
                pltpu.VMEM((2 * n, t, rep, hd), q.dtype),
                pltpu.VMEM((2 * n, hd, rep * t), q.dtype),
                pltpu.VMEM((hd, 2 * n * t), v.dtype),
                *[pltpu.VMEM((4 * t, rep * t), F32)] * 4,
                *[pltpu.VMEM((1, rep * t), F32)] * 4,
                pltpu.VMEM((2 * n, hd, rep * t), F32),
                pltpu.VMEM((2 * n, 1, rep * t), F32),
                pltpu.VMEM((2 * n, 1, rep * t), F32),
                pltpu.VMEM((2 * n, t, rep, hd), q.dtype),
                dma((8 * n,)), dma((1,)), dma((4 * n,)), dma((n,)),
                dma((2 * n - 2,)), dma((2 * n,)), dma((4 * n,)), dma((1,)),
            ],
            compiler_params=pltpu.CompilerParams(collective_id=0, has_side_effects=True,
                                                 vmem_limit_bytes=56 * 1024 * 1024),
        )(qh, k, v)
        return o.reshape(t, nh, hd)

    return jax.shard_map(local, mesh=mesh, in_specs=(spec, spec, spec), out_specs=spec, check_vma=False)
```

```python
import functools
import math

import jax
import jax.numpy as jnp
from jax import lax
from jax.experimental import pallas as pl
from jax.experimental.pallas import tpu as pltpu
from jax.sharding import PartitionSpec as P

NEG = -1.0e30
MESH = pl.DeviceIdType.MESH
F32 = jnp.float32


def kernel(n, c2, q_hbm, k_hbm, v_hbm, out_hbm, kraw, wide, ksend, ksem, kvbuf, qbuf, qt, vt, s0, s1, s2, s3, x0, x1, x2, x3, acc, mref, lref, ostage,
           ks, kr, qs, qr, gs, gr, os, orx):
    t2, ng, rep, hd = q_hbm.shape
    c = t2 // 2
    nb2 = 2 * n
    half = n * t2
    cols = rep * t2
    dp = lax.axis_index('dp')
    y = lax.axis_index('cy')
    cx = lax.axis_index('cx')
    x = cx // 2
    core = cx % 2
    row_core = core == 0
    own = jnp.where(row_core, y, x)
    pos = jnp.where(row_core, x, y)
    g_me = jnp.where(row_core, x, n + y)

    barrier = pltpu.get_barrier_semaphore()
    cnt = 0
    for d in range(1, 2 * n):
        pl.semaphore_signal(barrier, inc=1, device_id=(dp, y, (cx + d) % (2 * n)), device_id_type=MESH)
        cnt += 1
    for d in range(1, n):
        for cc in range(2):
            pl.semaphore_signal(barrier, inc=1, device_id=(dp, (y + d) % n, 2 * x + cc), device_id_type=MESH)
            cnt += 1

    loads = [pltpu.make_async_copy(src, kraw.at[w], ksem.at[w]) for w, src in enumerate((k_hbm, v_hbm))]
    for cp in loads:
        cp.start()
    for w, cp in enumerate(loads):
        cp.wait()
        wide[w] = kraw[w].astype(F32).reshape(t2 * ng, hd)
        for g in range(ng):
            ksend[w, g] = wide[w, pl.ds(g, t2, stride=ng), :].astype(jnp.bfloat16)
    pl.semaphore_wait(barrier, cnt)


    def spread(fn, sends, recv, split, parts, order):
        waits = []
        i = 0
        for d in order:
            for lay in range(2):
                u = x if lay == 0 else y
                j = (u + d) % n
                g = j + lay * n
                dev = (dp, y, 2 * j) if lay == 0 else (dp, j, 2 * x + 1)
                grp = y if lay == 0 else x
                for h in range(parts):
                    src, dst = fn(g, grp, u, h)
                    rsem = recv.at[u if split else 0]
                    cp = pltpu.make_async_remote_copy(src_ref=src, dst_ref=dst, send_sem=sends.at[i], recv_sem=rsem,
                                                      device_id=dev, device_id_type=MESH)
                    if d == 0:
                        lc = pltpu.make_async_copy(src, dst, rsem)
                        pl.when(core == lay)(lc.start)
                        pl.when(core != lay)(cp.start)
                        waits.append(lambda cp=cp, lay=lay: pl.when(core != lay)(cp.wait_send))
                    else:
                        cp.start()
                        waits.append(cp.wait_send)
                    i += 1
        return waits

    def kv_piece(g, grp, u, hw):
        h, w = hw % 2, hw // 2
        blk = u if h == 0 else nb2 - 1 - u
        sub = core if h == 0 else 1 - core
        off = pl.multiple_of(blk * t2 + sub * c, c)
        return ksend.at[w, g, pl.ds(h * c, c)], kvbuf.at[grp, w, pl.ds(off, c)]

    def q_piece(g, grp, u, h):
        blk = u if h == 0 else nb2 - 1 - u
        sub = core if h == 0 else 1 - core
        off = pl.multiple_of(sub * c, c)
        return q_hbm.at[pl.ds(h * c, c), g], qbuf.at[blk, pl.ds(off, c)]

    waits = spread(kv_piece, ks, kr, False, 4, (2, 1, 3, 0))
    waits += spread(q_piece, qs, qr, True, 2, (0, 1, 3, 2))

    def me_wait(ref, sem):
        pltpu.make_async_copy(ref, ref, sem).wait()

    def peer(p):
        return (dp, jnp.where(row_core, p, y), jnp.where(row_core, 2 * x, 2 * p + 1))

    def hand_on(t, h, d, sem):
        p = (own + d) % n
        part = kvbuf.at[t, :, pl.ds(h * half, half)]
        cp = pltpu.make_async_remote_copy(src_ref=part, dst_ref=part, send_sem=gs.at[sem], recv_sem=gr.at[2 * t + h],
                                          device_id=peer(p), device_id_type=MESH)
        return cp, True if h == 0 else jnp.logical_or(core == 1, t > p)

    def share_copies():
        return [hand_on(own, h, d, sem) for sem, (h, d) in enumerate(((0, 1), (1, n - 1), (1, 1), (0, n - 1)))]

    prev, after = (own + n - 1) % n, (own + 1) % n

    def relay_copies():
        return [hand_on(prev, 0, 1, 4), hand_on(after, 1, n - 1, 5)]

    def relay():
        for (cp, need), t, h in zip(relay_copies(), (prev, after), (0, 1)):
            @pl.when(need)
            def _(cp=cp, t=t, h=h):
                me_wait(kvbuf.at[t, :, pl.ds(h * half, half)], gr.at[2 * t + h])
                cp.start()

    def share():
        for cp, need in share_copies():
            pl.when(need)(cp.start)

    def turn_v(t, base):
        vt[:, pl.ds(base, half)] = kvbuf[t, 1, pl.ds(base, half), :].T

    s_bufs = (s0, s1, s2, s3)
    x_bufs = (x0, x1, x2, x3)

    def score(step, t, slot):
        q, b0, nb, diag, _ = step
        k = kvbuf[t, 0, pl.ds(b0 * t2, nb * t2), :]
        s = lax.dot_general(k, qt[q], (((1,), (0,)), ((), ())), preferred_element_type=F32)
        if diag:
            key = lax.broadcasted_iota(jnp.int32, (t2, cols), 0)
            row = lax.broadcasted_iota(jnp.int32, (t2, cols), 1) // rep
            tail = jnp.where(key <= row, s[(nb - 1) * t2:], NEG)
            s = tail if nb == 1 else jnp.concatenate([s[:(nb - 1) * t2], tail], axis=0)
        s_bufs[slot][pl.ds(0, nb * t2), :] = s
        x_bufs[slot][...] = jnp.max(s, axis=0, keepdims=True)

    def fold(step, slot):
        q, b0, nb, _, fresh = step
        s = s_bufs[slot][pl.ds(0, nb * t2), :]
        mx = x_bufs[slot][...]
        if not fresh:
            mp = mref[q]
            mx = jnp.maximum(mp, mx)
            alpha = jnp.exp2((mp - mx) * c2)
        mref[q] = mx
        p = jnp.exp2((s - mx) * c2)
        ls = jnp.sum(p, axis=0, keepdims=True)
        v = vt[:, pl.ds(b0 * t2, nb * t2)]
        pv = lax.dot_general(v, p.astype(jnp.bfloat16), (((1,), (0,)), ((), ())), preferred_element_type=F32)
        if fresh:
            lref[q] = ls
            acc[q] = pv
        else:
            lref[q] = alpha * lref[q] + ls
            acc[q] = alpha * acc[q] + pv

    def run(t, ranges, own_group):
        plan = []
        for q, b0, b1 in ranges:
            fresh = own_group
            while b0 < b1:
                nb = min(4, b1 - b0)
                plan.append((q, b0, nb, own_group and b0 + nb == b1, fresh))
                b0 += nb
                fresh = False
        for i in range(min(2, len(plan))):
            score(plan[i], t, i % 4)
        for i, step in enumerate(plan):
            if i + 2 < len(plan):
                score(plan[i + 2], t, (i + 2) % 4)
            fold(step, i % 4)

    def near(i):
        return jnp.where(i == 0, 0, jnp.where(i == 1, n - 1, i - 1))

    def finish(a):
        o = acc[a] * (1.0 / lref[a])
        ostage[a] = o.T.astype(jnp.bfloat16).reshape(t2, rep, hd)

    def o_copies(a, h):
        first_half = a < n
        u = jnp.where(first_half, a, nb2 - 1 - a)
        cc = jnp.where(first_half, h, 1 - h)
        dev = (dp, jnp.where(row_core, y, u), jnp.where(row_core, 2 * u, 2 * x) + cc)
        off = pl.multiple_of(jnp.where(first_half, 0, c), c)
        src = ostage.at[a, pl.ds(h * c, c)]
        dst = out_hbm.at[pl.ds(off, c), g_me]
        mine = jnp.logical_and(u == pos, cc == core)
        rc = pltpu.make_async_remote_copy(src_ref=src, dst_ref=dst, send_sem=os.at[2 * a + h], recv_sem=orx.at[0],
                                          device_id=dev, device_id_type=MESH)
        return mine, pltpu.make_async_copy(src, dst, orx.at[0]), rc

    def send_out(a):
        finish(a)
        for h in range(2):
            mine, lc, rc = o_copies(a, h)
            pl.when(mine)(lc.start)
            pl.when(jnp.logical_not(mine))(rc.start)

    def turn_q(u):
        me_wait(qbuf.at[pl.ds(0, 2)], qr.at[u])
        for blk in (u, nb2 - 1 - u):
            qt[blk] = qbuf[blk].reshape(cols, hd).T

    def reach(core_is, before, q):
        if core_is == 0:
            return (n if before else 0) if q < n else (n if before else nb2)
        return q + int(before == (q < n))

    def other(t, core_is, before, blocks, halves):
        ranges = []
        for q in blocks:
            for h in halves:
                ranges.append((q, h * n, min(reach(core_is, before, q), (h + 1) * n)))
        run(t, ranges, False)

    def each_form(t, fn, also=None):
        for core_is in range(2):
            for bf in (True, False):
                cond = jnp.logical_and(core == core_is, (t < own) == bf)
                pl.when(cond if also is None else jnp.logical_and(cond, also))(functools.partial(fn, core_is, bf))

    def send_range(lo, hi):
        lax.fori_loop(lo, hi, lambda q, c: (send_out(q), c)[1], 0)

    me_wait(kvbuf.at[own], kr.at[0])
    share()
    turn_v(own, 0)
    turn_v(own, half)
    def own_pair(i, carry):
        u = (pos + near(i)) % n
        turn_q(u)
        for k in range(n):
            @pl.when(u == k)
            def _(k=k):
                run(own, [(q, 0, q + 1) for q in (nb2 - 1 - k, k)], True)
        return carry

    lax.fori_loop(0, n, own_pair, 0)
    relay()

    def take(t, h, in_relay):
        base = pl.multiple_of(h * half, half)

        @pl.when(jnp.logical_or(h == 0, jnp.logical_or(core == 1, t > own)))
        def _():
            @pl.when(jnp.logical_not(in_relay))
            def _():
                me_wait(kvbuf.at[t, :, pl.ds(base, half)], gr.at[2 * t + h])
            turn_v(t, base)

    def phase(i, carry):
        t = (own + jnp.where(i % 2 == 0, n - 1, 1)) % n
        h = jnp.where(jnp.logical_or(i == 1, i == 2), 1, 0)
        take(t, h, jnp.logical_or(i == 0, jnp.logical_and(i == 1, jnp.logical_or(core == 1, after > prev))))
        for hh in range(2):
            each_form(t, lambda core_is, bf, hh=hh: other(t, core_is, bf, range(n * hh, nb2) if hh else range(nb2), (hh,)), h == hh)
        return carry

    lax.fori_loop(0, n, phase, 0)

    far = (own + 2) % n
    take(far, 0, core < 0)
    each_form(far, lambda core_is, bf: other(far, core_is, bf, range(n), (0,)))
    send_range(0, n)
    take(far, 1, core < 0)

    def tail(i, carry):
        w = jnp.where(pos < n // 2, i, 1 - i)
        for ww in range(2):
            lo = n + ww * (n // 2)
            each_form(far, lambda core_is, bf, lo=lo: other(far, core_is, bf, range(lo, lo + n // 2), (0, 1)), w == ww)
        send_range(n + w * (n // 2), n + (w + 1) * (n // 2))
        return carry

    lax.fori_loop(0, 2, tail, 0)

    for w in waits:
        w()
    for cp, need in share_copies() + relay_copies():
        pl.when(need)(cp.wait_send)

    def drain(a, carry):
        for h in range(2):
            mine, _, rc = o_copies(a, h)
            pl.when(jnp.logical_not(mine))(rc.wait_send)
        return carry

    lax.fori_loop(0, nb2, drain, 0)
    me_wait(out_hbm, orx.at[0])


def solution(mesh):
    n = mesh.shape['cy']
    assert n == 4 and mesh.shape['cx'] == 2 * n
    spec = P(('dp', 'cy', 'cx'))

    def local(q, k, v):
        t, nh, hd = q.shape
        ng = k.shape[1]
        assert ng == 2 * n
        rep = nh // ng
        c2 = hd ** -0.5 * math.log2(math.e)
        qh = q.reshape(t, ng, rep, hd)
        dma = pltpu.SemaphoreType.DMA
        o = pl.pallas_call(
            functools.partial(kernel, n, c2),
            out_shape=jax.ShapeDtypeStruct((t, ng, rep, hd), q.dtype),
            in_specs=[pl.BlockSpec(memory_space=pl.ANY)] * 3,
            out_specs=pl.BlockSpec(memory_space=pl.ANY),
            scratch_shapes=[
                pltpu.VMEM((2, t, ng, hd), k.dtype),
                pltpu.VMEM((2, t * ng, hd), F32),
                pltpu.VMEM((2, ng, t, hd), k.dtype),
                dma((2,)),
                pltpu.VMEM((n, 2, 2 * n * t, hd), k.dtype),
                pltpu.VMEM((2 * n, t, rep, hd), q.dtype),
                pltpu.VMEM((2 * n, hd, rep * t), q.dtype),
                pltpu.VMEM((hd, 2 * n * t), v.dtype),
                *[pltpu.VMEM((4 * t, rep * t), F32)] * 4,
                *[pltpu.VMEM((1, rep * t), F32)] * 4,
                pltpu.VMEM((2 * n, hd, rep * t), F32),
                pltpu.VMEM((2 * n, 1, rep * t), F32),
                pltpu.VMEM((2 * n, 1, rep * t), F32),
                pltpu.VMEM((2 * n, t, rep, hd), q.dtype),
                dma((8 * n,)), dma((1,)), dma((4 * n,)), dma((n,)),
                dma((2 * n - 2,)), dma((2 * n,)), dma((4 * n,)), dma((1,)),
            ],
            compiler_params=pltpu.CompilerParams(collective_id=0, has_side_effects=True,
                                                 vmem_limit_bytes=56 * 1024 * 1024),
        )(qh, k, v)
        return o.reshape(t, nh, hd)

    return jax.shard_map(local, mesh=mesh, in_specs=(spec, spec, spec), out_specs=spec, check_vma=False)
```

```python
import functools
import math

import jax
import jax.numpy as jnp
from jax import lax
from jax.experimental import pallas as pl
from jax.experimental.pallas import tpu as pltpu
from jax.sharding import PartitionSpec as P

NEG = -1.0e30
MESH = pl.DeviceIdType.MESH
F32 = jnp.float32


def kernel(n, c2, q_hbm, k_hbm, v_hbm, out_hbm, kraw, wide, ksend, ksem, kvbuf, qbuf, qt, vt, s0, s1, s2, s3, x0, x1, x2, x3, acc, mref, lref, ostage,
           ks, kr, qs, qr, gs, gr, os, orx):
    t2, ng, rep, hd = q_hbm.shape
    c = t2 // 2
    nb2 = 2 * n
    half = n * t2
    cols = rep * t2
    dp = lax.axis_index('dp')
    y = lax.axis_index('cy')
    cx = lax.axis_index('cx')
    x = cx // 2
    core = cx % 2
    row_core = core == 0
    own = jnp.where(row_core, y, x)
    pos = jnp.where(row_core, x, y)
    g_me = jnp.where(row_core, x, n + y)

    barrier = pltpu.get_barrier_semaphore()
    cnt = 0
    for d in range(1, 2 * n):
        pl.semaphore_signal(barrier, inc=1, device_id=(dp, y, (cx + d) % (2 * n)), device_id_type=MESH)
        cnt += 1
    for d in range(1, n):
        for cc in range(2):
            pl.semaphore_signal(barrier, inc=1, device_id=(dp, (y + d) % n, 2 * x + cc), device_id_type=MESH)
            cnt += 1

    loads = [pltpu.make_async_copy(src, kraw.at[w], ksem.at[w]) for w, src in enumerate((k_hbm, v_hbm))]
    for cp in loads:
        cp.start()
    for w, cp in enumerate(loads):
        cp.wait()
        wide[w] = kraw[w].astype(F32).reshape(t2 * ng, hd)
        for g in range(ng):
            ksend[w, g] = wide[w, pl.ds(g, t2, stride=ng), :].astype(jnp.bfloat16)
    pl.semaphore_wait(barrier, cnt)


    def spread(fn, sends, recv, split, parts, order):
        waits = []
        i = 0
        for d in order:
            for lay in range(2):
                u = x if lay == 0 else y
                j = (u + d) % n
                g = j + lay * n
                dev = (dp, y, 2 * j) if lay == 0 else (dp, j, 2 * x + 1)
                grp = y if lay == 0 else x
                for h in range(parts):
                    src, dst = fn(g, grp, u, h)
                    rsem = recv.at[u if split else 0]
                    cp = pltpu.make_async_remote_copy(src_ref=src, dst_ref=dst, send_sem=sends.at[i], recv_sem=rsem,
                                                      device_id=dev, device_id_type=MESH)
                    if d == 0:
                        lc = pltpu.make_async_copy(src, dst, rsem)
                        pl.when(core == lay)(lc.start)
                        pl.when(core != lay)(cp.start)
                        waits.append(lambda cp=cp, lay=lay: pl.when(core != lay)(cp.wait_send))
                    else:
                        cp.start()
                        waits.append(cp.wait_send)
                    i += 1
        return waits

    def kv_piece(g, grp, u, hw):
        h, w = hw % 2, hw // 2
        blk = u if h == 0 else nb2 - 1 - u
        sub = core if h == 0 else 1 - core
        off = pl.multiple_of(blk * t2 + sub * c, c)
        return ksend.at[w, g, pl.ds(h * c, c)], kvbuf.at[grp, w, pl.ds(off, c)]

    def q_piece(g, grp, u, h):
        blk = u if h == 0 else nb2 - 1 - u
        sub = core if h == 0 else 1 - core
        off = pl.multiple_of(sub * c, c)
        return q_hbm.at[pl.ds(h * c, c), g], qbuf.at[blk, pl.ds(off, c)]

    waits = spread(kv_piece, ks, kr, False, 4, (2, 1, 3, 0))
    waits += spread(q_piece, qs, qr, True, 2, (0, 1, 3, 2))

    def me_wait(ref, sem):
        pltpu.make_async_copy(ref, ref, sem).wait()

    def peer(p):
        return (dp, jnp.where(row_core, p, y), jnp.where(row_core, 2 * x, 2 * p + 1))

    def hand_on(t, h, d, sem):
        p = (own + d) % n
        part = kvbuf.at[t, :, pl.ds(h * half, half)]
        cp = pltpu.make_async_remote_copy(src_ref=part, dst_ref=part, send_sem=gs.at[sem], recv_sem=gr.at[2 * t + h],
                                          device_id=peer(p), device_id_type=MESH)
        return cp, True if h == 0 else jnp.logical_or(core == 1, t > p)

    def share_copies():
        return [hand_on(own, h, d, sem) for sem, (h, d) in enumerate(((0, 1), (1, n - 1), (1, 1), (0, n - 1)))]

    prev, after = (own + n - 1) % n, (own + 1) % n

    def relay_copies():
        return [hand_on(prev, 0, 1, 4), hand_on(after, 1, n - 1, 5)]

    def relay():
        for (cp, need), t, h in zip(relay_copies(), (prev, after), (0, 1)):
            @pl.when(need)
            def _(cp=cp, t=t, h=h):
                me_wait(kvbuf.at[t, :, pl.ds(h * half, half)], gr.at[2 * t + h])
                cp.start()

    def share():
        for cp, need in share_copies():
            pl.when(need)(cp.start)

    def turn_v(t, base):
        vt[:, pl.ds(base, half)] = kvbuf[t, 1, pl.ds(base, half), :].T

    s_bufs = (s0, s1, s2, s3)
    x_bufs = (x0, x1, x2, x3)

    def score(step, t, slot):
        q, b0, nb, diag, _ = step
        k = kvbuf[t, 0, pl.ds(b0 * t2, nb * t2), :]
        s = lax.dot_general(k, qt[q], (((1,), (0,)), ((), ())), preferred_element_type=F32)
        if diag:
            key = lax.broadcasted_iota(jnp.int32, (t2, cols), 0)
            row = lax.broadcasted_iota(jnp.int32, (t2, cols), 1) // rep
            tail = jnp.where(key <= row, s[(nb - 1) * t2:], NEG)
            s = tail if nb == 1 else jnp.concatenate([s[:(nb - 1) * t2], tail], axis=0)
        s_bufs[slot][pl.ds(0, nb * t2), :] = s
        x_bufs[slot][...] = jnp.max(s, axis=0, keepdims=True)

    def fold(step, slot):
        q, b0, nb, _, fresh = step
        s = s_bufs[slot][pl.ds(0, nb * t2), :]
        mx = x_bufs[slot][...]
        if not fresh:
            mp = mref[q]
            mx = jnp.maximum(mp, mx)
            alpha = jnp.exp2((mp - mx) * c2)
        mref[q] = mx
        p = jnp.exp2((s - mx) * c2)
        ls = jnp.sum(p, axis=0, keepdims=True)
        v = vt[:, pl.ds(b0 * t2, nb * t2)]
        pv = lax.dot_general(v, p.astype(jnp.bfloat16), (((1,), (0,)), ((), ())), preferred_element_type=F32)
        if fresh:
            lref[q] = ls
            acc[q] = pv
        else:
            lref[q] = alpha * lref[q] + ls
            acc[q] = alpha * acc[q] + pv

    def run(t, ranges, own_group):
        plan = []
        for q, b0, b1 in ranges:
            fresh = own_group
            while b0 < b1:
                nb = min(4, b1 - b0)
                plan.append((q, b0, nb, own_group and b0 + nb == b1, fresh))
                b0 += nb
                fresh = False
        for i in range(min(3, len(plan))):
            score(plan[i], t, i % 4)
        for i, step in enumerate(plan):
            if i + 3 < len(plan):
                score(plan[i + 3], t, (i + 3) % 4)
            fold(step, i % 4)

    def near(i):
        return jnp.where(i == 0, 0, jnp.where(i == 1, n - 1, i - 1))

    def finish(a):
        o = acc[a] * (1.0 / lref[a])
        ostage[a] = o.T.astype(jnp.bfloat16).reshape(t2, rep, hd)

    def o_copies(a, h):
        first_half = a < n
        u = jnp.where(first_half, a, nb2 - 1 - a)
        cc = jnp.where(first_half, h, 1 - h)
        dev = (dp, jnp.where(row_core, y, u), jnp.where(row_core, 2 * u, 2 * x) + cc)
        off = pl.multiple_of(jnp.where(first_half, 0, c), c)
        src = ostage.at[a, pl.ds(h * c, c)]
        dst = out_hbm.at[pl.ds(off, c), g_me]
        mine = jnp.logical_and(u == pos, cc == core)
        rc = pltpu.make_async_remote_copy(src_ref=src, dst_ref=dst, send_sem=os.at[2 * a + h], recv_sem=orx.at[0],
                                          device_id=dev, device_id_type=MESH)
        return mine, pltpu.make_async_copy(src, dst, orx.at[0]), rc

    def send_out(a):
        finish(a)
        for h in range(2):
            mine, lc, rc = o_copies(a, h)
            pl.when(mine)(lc.start)
            pl.when(jnp.logical_not(mine))(rc.start)

    def turn_q(u):
        me_wait(qbuf.at[pl.ds(0, 2)], qr.at[u])
        for blk in (u, nb2 - 1 - u):
            qt[blk] = qbuf[blk].reshape(cols, hd).T

    def reach(core_is, before, q):
        if core_is == 0:
            return (n if before else 0) if q < n else (n if before else nb2)
        return q + int(before == (q < n))

    def other(t, core_is, before, blocks, halves):
        ranges = []
        for q in blocks:
            for h in halves:
                ranges.append((q, h * n, min(reach(core_is, before, q), (h + 1) * n)))
        run(t, ranges, False)

    def each_form(t, fn, also=None):
        for core_is in range(2):
            for bf in (True, False):
                cond = jnp.logical_and(core == core_is, (t < own) == bf)
                pl.when(cond if also is None else jnp.logical_and(cond, also))(functools.partial(fn, core_is, bf))

    def send_range(lo, hi):
        lax.fori_loop(lo, hi, lambda q, c: (send_out(q), c)[1], 0)

    me_wait(kvbuf.at[own], kr.at[0])
    share()
    turn_v(own, 0)
    turn_v(own, half)
    def own_pair(i, carry):
        u = (pos + near(i)) % n
        turn_q(u)
        for k in range(n):
            @pl.when(u == k)
            def _(k=k):
                run(own, [(q, 0, q + 1) for q in (nb2 - 1 - k, k)], True)
        return carry

    lax.fori_loop(0, n, own_pair, 0)
    relay()

    def take(t, h, in_relay):
        base = pl.multiple_of(h * half, half)

        @pl.when(jnp.logical_or(h == 0, jnp.logical_or(core == 1, t > own)))
        def _():
            @pl.when(jnp.logical_not(in_relay))
            def _():
                me_wait(kvbuf.at[t, :, pl.ds(base, half)], gr.at[2 * t + h])
            turn_v(t, base)

    def phase(i, carry):
        t = (own + jnp.where(i % 2 == 0, n - 1, 1)) % n
        h = jnp.where(jnp.logical_or(i == 1, i == 2), 1, 0)
        take(t, h, jnp.logical_or(i == 0, jnp.logical_and(i == 1, jnp.logical_or(core == 1, after > prev))))
        for hh in range(2):
            each_form(t, lambda core_is, bf, hh=hh: other(t, core_is, bf, range(n * hh, nb2) if hh else range(nb2), (hh,)), h == hh)
        return carry

    lax.fori_loop(0, n, phase, 0)

    far = (own + 2) % n
    take(far, 0, core < 0)
    each_form(far, lambda core_is, bf: other(far, core_is, bf, range(n), (0,)))
    send_range(0, n)
    take(far, 1, core < 0)

    def tail(i, carry):
        w = jnp.where(pos < n // 2, i, 1 - i)
        for ww in range(2):
            lo = n + ww * (n // 2)
            each_form(far, lambda core_is, bf, lo=lo: other(far, core_is, bf, range(lo, lo + n // 2), (0, 1)), w == ww)
        send_range(n + w * (n // 2), n + (w + 1) * (n // 2))
        return carry

    lax.fori_loop(0, 2, tail, 0)

    for w in waits:
        w()
    for cp, need in share_copies() + relay_copies():
        pl.when(need)(cp.wait_send)

    def drain(a, carry):
        for h in range(2):
            mine, _, rc = o_copies(a, h)
            pl.when(jnp.logical_not(mine))(rc.wait_send)
        return carry

    lax.fori_loop(0, nb2, drain, 0)
    me_wait(out_hbm, orx.at[0])


def solution(mesh):
    n = mesh.shape['cy']
    assert n == 4 and mesh.shape['cx'] == 2 * n
    spec = P(('dp', 'cy', 'cx'))

    def local(q, k, v):
        t, nh, hd = q.shape
        ng = k.shape[1]
        assert ng == 2 * n
        rep = nh // ng
        c2 = hd ** -0.5 * math.log2(math.e)
        qh = q.reshape(t, ng, rep, hd)
        dma = pltpu.SemaphoreType.DMA
        o = pl.pallas_call(
            functools.partial(kernel, n, c2),
            out_shape=jax.ShapeDtypeStruct((t, ng, rep, hd), q.dtype),
            in_specs=[pl.BlockSpec(memory_space=pl.ANY)] * 3,
            out_specs=pl.BlockSpec(memory_space=pl.ANY),
            scratch_shapes=[
                pltpu.VMEM((2, t, ng, hd), k.dtype),
                pltpu.VMEM((2, t * ng, hd), F32),
                pltpu.VMEM((2, ng, t, hd), k.dtype),
                dma((2,)),
                pltpu.VMEM((n, 2, 2 * n * t, hd), k.dtype),
                pltpu.VMEM((2 * n, t, rep, hd), q.dtype),
                pltpu.VMEM((2 * n, hd, rep * t), q.dtype),
                pltpu.VMEM((hd, 2 * n * t), v.dtype),
                *[pltpu.VMEM((4 * t, rep * t), F32)] * 4,
                *[pltpu.VMEM((1, rep * t), F32)] * 4,
                pltpu.VMEM((2 * n, hd, rep * t), F32),
                pltpu.VMEM((2 * n, 1, rep * t), F32),
                pltpu.VMEM((2 * n, 1, rep * t), F32),
                pltpu.VMEM((2 * n, t, rep, hd), q.dtype),
                dma((8 * n,)), dma((1,)), dma((4 * n,)), dma((n,)),
                dma((2 * n - 2,)), dma((2 * n,)), dma((4 * n,)), dma((1,)),
            ],
            compiler_params=pltpu.CompilerParams(collective_id=0, has_side_effects=True,
                                                 vmem_limit_bytes=56 * 1024 * 1024),
        )(qh, k, v)
        return o.reshape(t, nh, hd)

    return jax.shard_map(local, mesh=mesh, in_specs=(spec, spec, spec), out_specs=spec, check_vma=False)
```
